32 devices in a mesh: gx: 8 (over y, x, core), gy: 4 (over z).
Axes of the slice: x: 2, y: 2, z: 4, core: 2. Of those that a mesh axis runs over, the one named last changes fastest.
Arguments:
- probes: float32 [16, 128, 128, 256], P(None, 'gx', 'gy'), may hold values from -6 to 6
- diffusivity: float32 [128, 128, 256], P('gx', 'gy'), may hold values from 0.5 to 2
- wind_speed: float32 [3], replicated, may hold values from 0.5 to 2
- sensor_cell: int32 [8, 4, 128], P('gx', 'gy'), may hold values from 0 to 131071
- sensor_owner: int32 [8, 4, 128, 1], P('gx', 'gy'), may hold values from 0 to 31; in each aligned block of 128 rows (0 to 127, 128 to 255, ..., all dimensions but the last counted through in order) at most 4 rows name the same one
- sensor_count: int32 [8, 4], P('gx', 'gy'), may hold values from 64 to 128
- goal_weight: float32 [8, 4, 128, 16], P('gx', 'gy'), may hold values from -0.6 to 0.6
Outputs:
- fields: float32 [16, 128, 128, 256], P(None, 'gx', 'gy')
- goal_block: float32 [512, 16], P(('gx', 'gy'))
- ritz_gram: float32 [16, 16], replicated
The draws below stay inside these ranges and needn't reach their ends.
Inputs may be any that keep to these rules, and one draw needn't show every extreme that they name: `sensor_owner`: among the rows of one device, no owner is named more than 4 times, a bound that some block reaches.
All inputs are finite; a program needn't handle non-finite values.
Results may differ from the reference program's by a relative error of at most 0.0003.
Values sent between devices are 32-bit elements; how exact they have to be, the bound alone decides.
A program may use at most 192 MiB of HBM per device.

```python
import math
import jax
import jax.numpy as jnp
import numpy as np
from jax import lax

CX = 16
CY = 32
CZ = 256
PROBES = 16
STEPS = 2
SWEEPS = 4
SENS = 128
CAP = 4
GOAL_DEV = 16
NX = 128
NY = 128
N_GX = 8
N_GY = 4


def place_ends(result, own_key, low, high):
    longest = result.shape.index(max(result.shape))
    spots = []
    for shift in (0, 1):
        where = [jax.random.randint(jax.random.fold_in(own_key, axis), (), 0, length) for axis, length in enumerate(result.shape)]
        where[longest] = (where[longest] + shift) % result.shape[longest]
        spots.append(tuple(where))
    return result.at[spots[0]].set(low).at[spots[1]].set(high)


def level_of(own_key, extent, cuts, least, high):
    def one(dim, parts):
        draws = jax.random.uniform(jax.random.fold_in(jax.random.fold_in(own_key, 6), dim), (parts,), jnp.float32, least / len(cuts), high / len(cuts))
        return jnp.repeat(jnp.exp(draws), extent[dim] // parts).reshape((-1,) + (1,) * (len(extent) - dim - 1))

    gain = one(*cuts[0])
    for cut in cuts[1:]:
        gain = gain * one(*cut)
    return gain


def shared_out(own_key, own, number, rows, count, top, bound, slope):
    ranking = jax.random.permutation(own_key, count)
    packed, common = shares(count, rows * top, bound, slope, True), shares(count, rows * top, bound, slope, False)
    places = jnp.arange(count)

    def named(lengths, turn):
        used = int((lengths > 0).sum())
        fixed = max(1, used // 4)
        shifted = fixed + (places - fixed + turn * (used - fixed)) % max(1, count - fixed)
        return jnp.zeros((count,), jnp.int32).at[ranking[jnp.where(places < fixed, places, shifted)]].set(jnp.asarray(lengths, jnp.int32))

    lengths = jnp.where(number % 4 == 0, named(packed, number // 4), named(common, number - number // 4 - 1))
    mixed = jax.random.permutation(jax.random.fold_in(own, 3), count)
    donor, sink = mixed[0:count // 2 * 2:2], mixed[1:count // 2 * 2:2]
    slack = jnp.minimum(lengths[donor] - 1, bound - lengths[sink]) // 2
    slack = jnp.where((donor == ranking[0]) | (sink == ranking[0]) | (lengths[sink] == 0), 0, jnp.maximum(slack, 0))
    shifted = jax.random.randint(jax.random.fold_in(own, 4), (count // 2,), 0, 1 << 20) % (slack + 1)
    lengths = lengths.at[donor].add(-shifted).at[sink].add(shifted)
    members = jnp.searchsorted(jnp.cumsum(lengths), jnp.arange(rows * top), side="right").astype(jnp.int32)
    table = members.reshape(top, rows).T
    table = table[jax.random.permutation(jax.random.fold_in(own, 1), rows)]
    turn = jax.random.randint(jax.random.fold_in(own, 2), (rows, 1), 0, top)
    return jnp.take_along_axis(table, (jnp.arange(top)[None, :] + turn) % top, axis=1)


def shares(number_of, total, limit, slope, full):
    weights = [(1 << 20) // math.isqrt(rank ** slope) + 1 for rank in range(1, number_of + 1)]
    largest = limit if full else min(limit, max(-(-total // number_of), total * weights[0] // sum(weights)))
    least = 1 if total - largest >= number_of - 1 else 0
    given, rest = [largest] + [least] * (number_of - 1), total - largest - least * (number_of - 1)
    while rest > 0:
        movable = [i for i in range(1, number_of) if given[i] < largest] or [i for i in range(1, number_of) if given[i] < limit]
        whole, left = sum([weights[i] for i in movable]), rest
        for i in movable:
            extra = min(limit - given[i], max(1, left * weights[i] // whole), rest)
            given[i] = given[i] + extra
            rest = rest - extra
    return np.array(given)


def centred(key, extent, spread, reach, cuts=(), held_as=jnp.bfloat16):
    level = level_of(key, extent, cuts, -0.22, 0.18) if cuts else 1.0
    entries = jax.random.normal(key, extent, jnp.float32) * spread * level
    return jnp.minimum(jnp.maximum(entries, -reach), reach).astype(held_as)


def setup_inputs(seed: int = 0) -> dict:
    arg_keys = jax.random.split(jax.random.key(seed), 8)
    probes = centred(arg_keys[0], (PROBES, NX, NY, CZ), 1.0, 6.0, ((1, 8), (2, 4)), jnp.float32)
    diffusivity = jnp.clip(jnp.exp(math.log(2.0) - 1.3862944 * jax.random.uniform(arg_keys[1], (NX, NY, CZ), jnp.float32) ** level_of(arg_keys[1], (NX, NY, CZ), ((0, 8), (1, 4)), -0.2, 0.2)), 0.5, 2.0)
    wind_speed = jnp.clip(jax.random.uniform(arg_keys[2], (3,), jnp.float32, 0.5, 2.0), 0.5, 2.0)
    sensor_cell = place_ends(jax.random.randint(arg_keys[3], (N_GX, N_GY, SENS), 0, CX * CY * CZ), jax.random.fold_in(arg_keys[3], 1), 0, (CX * CY * CZ) - 1).astype(jnp.int32)
    sensor_owner_keys = jax.random.split(jax.random.fold_in(arg_keys[4], 1), N_GX * N_GY * SENS // SENS)
    sensor_owner_turns = jax.random.permutation(jax.random.fold_in(arg_keys[4], 3), N_GX * N_GY * SENS // SENS)
    sensor_owner = jax.vmap(lambda own, number: shared_out(jax.random.fold_in(arg_keys[4], 2), own, number, SENS, N_GX * N_GY, 1, CAP, 1))(sensor_owner_keys, sensor_owner_turns).reshape((N_GX, N_GY, SENS, 1))
    sensor_count = place_ends(jax.random.randint(arg_keys[5], (N_GX, N_GY), SENS // 2, SENS + 1), jax.random.fold_in(arg_keys[5], 1), SENS // 2, SENS).astype(jnp.int32)
    goal_weight = centred(arg_keys[6], (N_GX, N_GY, SENS, GOAL_DEV), 0.1, 0.6, ((0, 8), (1, 4)), jnp.float32)
    return dict(probes=probes, diffusivity=diffusivity, wind_speed=wind_speed, sensor_cell=sensor_cell, sensor_owner=sensor_owner, sensor_count=sensor_count, goal_weight=goal_weight)


time_step = 2.0


def relax(padded, source, diffusion, wind_speed):
    centre = padded[..., 1:-1, 1:-1, :]
    widths = [(0, 0)] * (centre.ndim - 1) + [(1, 1)]
    zpadded = jnp.pad(centre, widths)
    beside = padded[..., 2:, 1:-1, :] + padded[..., :-2, 1:-1, :]
    beside = beside + padded[..., 1:-1, 2:, :] + padded[..., 1:-1, :-2, :]
    beside = beside + zpadded[..., 2:] + zpadded[..., :-2]
    upwind = wind_speed[0] * padded[..., :-2, 1:-1, :] + wind_speed[1] * padded[..., 1:-1, :-2, :] + wind_speed[2] * zpadded[..., :-2]
    diagonal = 1.0 + time_step * (6.0 * diffusion + wind_speed[0] + wind_speed[1] + wind_speed[2])
    updated = (source + time_step * (diffusion * beside + upwind)) / diagonal
    return jnp.where(diffusion > 0.0, updated, 0.0)


def reference(probes, diffusivity, wind_speed, sensor_cell, sensor_owner, sensor_count, goal_weight):
    def advance(state_field):
        for step_index in range(STEPS):
            source = state_field
            for sweep_index in range(SWEEPS):
                state_field = relax(jnp.pad(state_field, ((1, 1), (1, 1), (0, 0))), source, diffusivity, wind_speed)
        return state_field

    fields = lax.map(advance, probes)
    blocks = fields.reshape(PROBES, N_GX, CX, N_GY, CY, CZ).transpose(1, 3, 0, 2, 4, 5)
    blocks = blocks.reshape(N_GX, N_GY, PROBES, CX * CY * CZ)
    readings = jnp.take_along_axis(blocks, sensor_cell[:, :, None, :].astype(jnp.int32), axis=3)
    active = (jnp.arange(SENS, dtype=jnp.int32)[None, None, :] < sensor_count[:, :, None]).astype(jnp.float32)
    readings = readings.transpose(0, 1, 3, 2) * active[..., None]
    outer = (goal_weight[..., :, None] * readings[..., None, :]).reshape(N_GX * N_GY * SENS, GOAL_DEV * PROBES)
    owners = sensor_owner.reshape(-1)
    onehot = (owners[:, None] == jnp.arange(N_GX * N_GY, dtype=jnp.int32)[None, :]).astype(jnp.float32)
    goal_block = jnp.dot(onehot.T, outer, precision=lax.Precision.HIGHEST).reshape(N_GX * N_GY * GOAL_DEV, PROBES)
    ritz_gram = jnp.dot(goal_block.T, goal_block, precision=lax.Precision.HIGHEST)
    return fields, goal_block, ritz_gram
```

```python
import jax
import jax.numpy as jnp
from jax import lax
from jax.experimental import pallas as pl
from jax.experimental.pallas import tpu as pltpu
from jax.sharding import PartitionSpec as P

STEPS = 2
SWEEPS = 4

time_step = 2.0

LANES = 8
CHUNK = 4


def schedule():
    plan, read = [], 0
    for _ in range(STEPS):
        source = read
        others = [b for b in range(3) if b != source]
        for k in range(SWEEPS):
            written = others[k % 2]
            plan.append((read, source, written))
            read = written
    return plan


def sweeps_kernel(wind, field, inverse, mixing, out, held, inv, mix, load_sem, store_sem, send_sem, recv_sem):
    groups, nx, ny = field.shape[0], field.shape[1], field.shape[2]
    nz = field.shape[4]
    gx, gy = lax.axis_index("gx"), lax.axis_index("gy")
    n_gx, n_gy = lax.axis_size("gx"), lax.axis_size("gy")
    xs, ys = pl.ds(1, nx), pl.ds(1, ny)

    loads = [pltpu.make_async_copy(field.at[g], held.at[0, g, xs, ys], load_sem.at[g]) for g in range(groups)]
    loads.append(pltpu.make_async_copy(inverse, inv, load_sem.at[groups]))
    loads.append(pltpu.make_async_copy(mixing, mix, load_sem.at[groups + 1]))
    for copy in loads:
        copy.start()

    row = jnp.zeros((ny + 2, LANES, nz), jnp.float32)
    for b in range(3):
        for g in range(groups):
            held[b, g, 0] = row
            held[b, g, nx + 1] = row
            held[b, g, xs, 0] = row[:nx] if nx <= ny + 2 else jnp.zeros((nx, LANES, nz), jnp.float32)
            held[b, g, xs, ny + 1] = row[:nx] if nx <= ny + 2 else jnp.zeros((nx, LANES, nz), jnp.float32)

    routes = (
        (gx < n_gx - 1, gx > 0, (gx + 1, gy)),
        (gx > 0, gx < n_gx - 1, (gx - 1, gy)),
        (gy < n_gy - 1, gy > 0, (gx, gy + 1)),
        (gy > 0, gy < n_gy - 1, (gx, gy - 1)),
    )
    barrier = pltpu.get_barrier_semaphore()
    for there, _, target in routes:
        @pl.when(there)
        def _():
            pl.semaphore_signal(barrier, inc=1, device_id=target, device_id_type=pl.DeviceIdType.MESH)
    peers = sum(there.astype(jnp.int32) for there, _, _ in routes)
    pl.semaphore_wait(barrier, peers)

    def face(d, b, g, turn):
        if d == 0:
            src, dst = held.at[b, g, nx, ys], held.at[b, g, 0, ys]
        elif d == 1:
            src, dst = held.at[b, g, 1, ys], held.at[b, g, nx + 1, ys]
        elif d == 2:
            src, dst = held.at[b, g, xs, ny], held.at[b, g, xs, 0]
        else:
            src, dst = held.at[b, g, xs, 1], held.at[b, g, xs, ny + 1]
        return pltpu.make_async_remote_copy(
            src_ref=src,
            dst_ref=dst,
            send_sem=send_sem.at[turn % 2, g, d],
            recv_sem=recv_sem.at[turn % 2, g, d],
            device_id=routes[d][2],
            device_id_type=pl.DeviceIdType.MESH,
        )

    def start(d, b, g, turn):
        @pl.when(routes[d][0])
        def _():
            face(d, b, g, turn).start()

    def wait_send(d, b, g, turn):
        @pl.when(routes[d][0])
        def _():
            face(d, b, g, turn).wait_send()

    def wait_recv(d, b, g, turn):
        @pl.when(routes[d][1])
        def _():
            face(d, b, g, turn).wait_recv()

    w0, w1, w2 = wind[0], wind[1], wind[2]
    lane = lax.broadcasted_iota(jnp.int32, (CHUNK, LANES, nz), 2)

    def plane(x, g, read, source, written):
        def chunk(k, carry):
            y = 1 + k * CHUNK
            centre = held[read, g, x, pl.ds(y, CHUNK)]
            x_low = held[read, g, x - 1, pl.ds(y, CHUNK)]
            x_high = held[read, g, x + 1, pl.ds(y, CHUNK)]
            y_low = held[read, g, x, pl.ds(y - 1, CHUNK)]
            y_high = held[read, g, x, pl.ds(y + 1, CHUNK)]
            z_low = jnp.where(lane == 0, 0.0, pltpu.roll(centre, 1, 2))
            z_high = jnp.where(lane == nz - 1, 0.0, pltpu.roll(centre, nz - 1, 2))
            beside = (x_low + x_high) + (y_low + y_high) + (z_low + z_high)
            upwind = w0 * x_low + w1 * y_low + w2 * z_low
            start_value = held[source, g, x, pl.ds(y, CHUNK)]
            r = inv[x - 1, pl.ds(y - 1, CHUNK)]
            a = mix[x - 1, pl.ds(y - 1, CHUNK)]
            held[written, g, x, pl.ds(y, CHUNK)] = (start_value + upwind) * r + a * beside
            return carry

        lax.fori_loop(0, ny // CHUNK, chunk, 0)

    plan = schedule()
    last = len(plan)
    for g in range(groups):
        loads[g].wait()
        for d in range(4):
            start(d, 0, g, 0)
    loads[groups].wait()
    loads[groups + 1].wait()

    stores = []
    for turn, (read, source, written) in enumerate(plan, 1):
        for g in range(groups):
            for d in range(4):
                wait_recv(d, read, g, turn - 1)
                if turn >= 2:
                    wait_send(d, plan[turn - 3][2] if turn >= 3 else 0, g, turn - 2)
            ends = (1, nx) if nx > 1 else (1,)
            for x in ends:
                plane(x, g, read, source, written)
            if turn < last:
                for d in (0, 1):
                    start(d, written, g, turn)

            def inner(x, carry):
                plane(x, g, read, source, written)
                return carry

            lax.fori_loop(2, nx, inner, 0)
            if turn < last:
                for d in (2, 3):
                    start(d, written, g, turn)
            else:
                stores.append(pltpu.make_async_copy(held.at[written, g, xs, ys], out.at[g], store_sem.at[g]))
                stores[-1].start()
    for g in range(groups):
        for d in range(4):
            wait_send(d, plan[last - 1][0], g, last - 1)
        stores[g].wait()


def run_sweeps(wind, field, inverse, mixing):
    groups, nx, ny, _, nz = field.shape
    hbm = pl.BlockSpec(memory_space=pl.ANY)
    return pl.pallas_call(
        sweeps_kernel,
        out_shape=jax.ShapeDtypeStruct(field.shape, jnp.float32),
        in_specs=[pl.BlockSpec(memory_space=pltpu.SMEM), hbm, hbm, hbm],
        out_specs=hbm,
        scratch_shapes=[
            pltpu.VMEM((3, groups, nx + 2, ny + 2, LANES, nz), jnp.float32),
            pltpu.VMEM((nx, ny, LANES, nz), jnp.float32),
            pltpu.VMEM((nx, ny, LANES, nz), jnp.float32),
            pltpu.SemaphoreType.DMA((groups + 2,)),
            pltpu.SemaphoreType.DMA((groups,)),
            pltpu.SemaphoreType.DMA((2, groups, 4)),
            pltpu.SemaphoreType.DMA((2, groups, 4)),
        ],
        compiler_params=pltpu.CompilerParams(
            collective_id=0, has_side_effects=True, vmem_limit_bytes=60 * 1024 * 1024
        ),
    )(wind, field, inverse, mixing)


def body(probes, diffusivity, wind_speed, sensor_cell, sensor_owner, sensor_count, goal_weight):
    probe_count, nx, ny, nz = probes.shape
    groups = probe_count // LANES
    field = probes.reshape(groups, LANES, nx, ny, nz).transpose(0, 2, 3, 1, 4)
    inverse = 1.0 / (
        1.0 + time_step * (6.0 * diffusivity + wind_speed[0] + wind_speed[1] + wind_speed[2])
    )
    mixing = time_step * diffusivity * inverse
    wide = (nx, ny, LANES, nz)
    state = run_sweeps(
        time_step * wind_speed,
        field,
        jnp.broadcast_to(inverse[:, :, None, :], wide),
        jnp.broadcast_to(mixing[:, :, None, :], wide),
    )
    fields = state.transpose(0, 3, 1, 2, 4).reshape(probes.shape)

    sensor_rows = sensor_cell.shape[2]
    goal_count = goal_weight.shape[3]
    device_count = lax.axis_size("gx") * lax.axis_size("gy")
    cells = sensor_cell.reshape(-1)
    columns = jnp.take(state.reshape(groups, nx * ny, LANES, nz), cells // nz, axis=1, mode="clip")
    here = jnp.arange(nz, dtype=jnp.int32)[None, :] == (cells % nz)[:, None]
    readings = jnp.sum(jnp.where(here[None, :, None, :], columns, 0.0), axis=3)
    readings = readings.transpose(1, 0, 2).reshape(sensor_rows, probe_count)
    active = jnp.arange(sensor_rows, dtype=jnp.int32) < sensor_count.reshape(())
    readings = jnp.where(active[:, None], readings, 0.0)
    payload = jnp.concatenate(
        [
            readings,
            goal_weight.reshape(sensor_rows, goal_count),
            sensor_owner.reshape(sensor_rows, 1).astype(jnp.float32),
        ],
        axis=1,
    )
    everyone = lax.all_gather(payload, ("gx", "gy"), axis=0, tiled=True)
    all_readings = everyone[:, :probe_count]
    all_weights = everyone[:, probe_count : probe_count + goal_count]
    owners = everyone[:, probe_count + goal_count].astype(jnp.int32)
    onehot = (owners[:, None] == jnp.arange(device_count, dtype=jnp.int32)[None, :]).astype(jnp.float32)
    outer = (all_weights[:, :, None] * all_readings[:, None, :]).reshape(-1, goal_count * probe_count)
    goals = jnp.dot(onehot.T, outer, precision=lax.Precision.HIGHEST)
    goals = goals.reshape(device_count * goal_count, probe_count)
    ritz_gram = jnp.dot(goals.T, goals, precision=lax.Precision.HIGHEST)
    mine = lax.axis_index("gx") * lax.axis_size("gy") + lax.axis_index("gy")
    goal_block = lax.dynamic_slice_in_dim(goals, mine * goal_count, goal_count, axis=0)
    return (fields, goal_block, ritz_gram)


def solution(mesh):
    placed = (
        P(None, "gx", "gy", None),
        P("gx", "gy", None),
        P(),
        P("gx", "gy", None),
        P("gx", "gy", None, None),
        P("gx", "gy"),
        P("gx", "gy", None, None),
    )
    return jax.shard_map(
        body,
        mesh=mesh,
        in_specs=placed,
        out_specs=(P(None, "gx", "gy", None), P(("gx", "gy"), None), P()),
        check_vma=False,
    )
```

```python
import jax
import jax.numpy as jnp
from jax import lax
from jax.experimental import pallas as pl
from jax.experimental.pallas import tpu as pltpu
from jax.sharding import PartitionSpec as P

STEPS = 2
SWEEPS = 4

time_step = 2.0

LANES = 8
CHUNK = 4


def schedule():
    plan, read = [], 0
    for _ in range(STEPS):
        source = read
        others = [b for b in range(3) if b != source]
        for k in range(SWEEPS):
            written = others[k % 2]
            plan.append((read, source, written))
            read = written
    return plan


def sweeps_kernel(wind, field, inverse, mixing, out, held0, held1, held2, inv, mix, load_sem, store_sem, send_sem, recv_sem):
    held = (held0, held1, held2)
    groups, nx, ny = field.shape[0], field.shape[1], field.shape[2]
    nz = field.shape[4]
    gx, gy = lax.axis_index("gx"), lax.axis_index("gy")
    n_gx, n_gy = lax.axis_size("gx"), lax.axis_size("gy")
    xs, ys = pl.ds(1, nx), pl.ds(1, ny)

    loads = [pltpu.make_async_copy(field.at[g], held[0].at[g, xs, ys], load_sem.at[g]) for g in range(groups)]
    loads.append(pltpu.make_async_copy(inverse, inv, load_sem.at[groups]))
    loads.append(pltpu.make_async_copy(mixing, mix, load_sem.at[groups + 1]))
    for copy in loads:
        copy.start()

    row = jnp.zeros((ny + 2, LANES, nz), jnp.float32)
    for b in range(3):
        for g in range(groups):
            held[b][g, 0] = row
            held[b][g, nx + 1] = row
            held[b][g, xs, 0] = row[:nx] if nx <= ny + 2 else jnp.zeros((nx, LANES, nz), jnp.float32)
            held[b][g, xs, ny + 1] = row[:nx] if nx <= ny + 2 else jnp.zeros((nx, LANES, nz), jnp.float32)

    routes = (
        (gx < n_gx - 1, gx > 0, (gx + 1, gy)),
        (gx > 0, gx < n_gx - 1, (gx - 1, gy)),
        (gy < n_gy - 1, gy > 0, (gx, gy + 1)),
        (gy > 0, gy < n_gy - 1, (gx, gy - 1)),
    )
    barrier = pltpu.get_barrier_semaphore()
    for there, _, target in routes:
        @pl.when(there)
        def _():
            pl.semaphore_signal(barrier, inc=1, device_id=target, device_id_type=pl.DeviceIdType.MESH)
    peers = sum(there.astype(jnp.int32) for there, _, _ in routes)
    pl.semaphore_wait(barrier, peers)

    def face(d, b, g, turn):
        if d == 0:
            src, dst = held[b].at[g, nx, ys], held[b].at[g, 0, ys]
        elif d == 1:
            src, dst = held[b].at[g, 1, ys], held[b].at[g, nx + 1, ys]
        elif d == 2:
            src, dst = held[b].at[g, xs, ny], held[b].at[g, xs, 0]
        else:
            src, dst = held[b].at[g, xs, 1], held[b].at[g, xs, ny + 1]
        return pltpu.make_async_remote_copy(
            src_ref=src,
            dst_ref=dst,
            send_sem=send_sem.at[turn % 2, g, d],
            recv_sem=recv_sem.at[turn % 2, g, d],
            device_id=routes[d][2],
            device_id_type=pl.DeviceIdType.MESH,
        )

    def start(d, b, g, turn):
        @pl.when(routes[d][0])
        def _():
            face(d, b, g, turn).start()

    def wait_send(d, b, g, turn):
        @pl.when(routes[d][0])
        def _():
            face(d, b, g, turn).wait_send()

    def wait_recv(d, b, g, turn):
        @pl.when(routes[d][1])
        def _():
            face(d, b, g, turn).wait_recv()

    w0, w1, w2 = wind[0], wind[1], wind[2]
    lane = lax.broadcasted_iota(jnp.int32, (CHUNK, LANES, nz), 2)

    def plane(x, g, read, source, written):
        for y in range(1, ny + 1, CHUNK):
            centre = held[read][g, x, pl.ds(y, CHUNK)]
            x_low = held[read][g, x - 1, pl.ds(y, CHUNK)]
            x_high = held[read][g, x + 1, pl.ds(y, CHUNK)]
            y_low = held[read][g, x, pl.ds(y - 1, CHUNK)]
            y_high = held[read][g, x, pl.ds(y + 1, CHUNK)]
            z_low = jnp.where(lane == 0, 0.0, pltpu.roll(centre, 1, 2))
            z_high = jnp.where(lane == nz - 1, 0.0, pltpu.roll(centre, nz - 1, 2))
            beside = (x_low + x_high) + (y_low + y_high) + (z_low + z_high)
            upwind = w0 * x_low + w1 * y_low + w2 * z_low
            start_value = held[source][g, x, pl.ds(y, CHUNK)]
            r = inv[x - 1, pl.ds(y - 1, CHUNK)]
            a = mix[x - 1, pl.ds(y - 1, CHUNK)]
            held[written][g, x, pl.ds(y, CHUNK)] = (start_value + upwind) * r + a * beside

    plan = schedule()
    last = len(plan)
    for g in range(groups):
        loads[g].wait()
        for d in range(4):
            start(d, 0, g, 0)
    loads[groups].wait()
    loads[groups + 1].wait()

    stores = []
    for turn, (read, source, written) in enumerate(plan, 1):
        for g in range(groups):
            for d in range(4):
                wait_recv(d, read, g, turn - 1)
                if turn >= 2:
                    wait_send(d, plan[turn - 3][2] if turn >= 3 else 0, g, turn - 2)
            def end(i, carry):
                plane(1 + i * (nx - 1), g, read, source, written)
                return carry

            lax.fori_loop(0, 2, end, 0)
            if turn < last:
                for d in (0, 1):
                    start(d, written, g, turn)

            def inner(x, carry):
                plane(x, g, read, source, written)
                return carry

            lax.fori_loop(2, nx, inner, 0)
            if turn < last:
                for d in (2, 3):
                    start(d, written, g, turn)
            else:
                stores.append(pltpu.make_async_copy(held[written].at[g, xs, ys], out.at[g], store_sem.at[g]))
                stores[-1].start()
    for g in range(groups):
        for d in range(4):
            wait_send(d, plan[last - 1][0], g, last - 1)
        stores[g].wait()


def run_sweeps(wind, field, inverse, mixing):
    groups, nx, ny, _, nz = field.shape
    hbm = pl.BlockSpec(memory_space=pl.ANY)
    return pl.pallas_call(
        sweeps_kernel,
        out_shape=jax.ShapeDtypeStruct(field.shape, jnp.float32),
        in_specs=[pl.BlockSpec(memory_space=pltpu.SMEM), hbm, hbm, hbm],
        out_specs=hbm,
        scratch_shapes=[
            *[pltpu.VMEM((groups, nx + 2, ny + 2, LANES, nz), jnp.float32)] * 3,
            pltpu.VMEM((nx, ny, LANES, nz), jnp.float32),
            pltpu.VMEM((nx, ny, LANES, nz), jnp.float32),
            pltpu.SemaphoreType.DMA((groups + 2,)),
            pltpu.SemaphoreType.DMA((groups,)),
            pltpu.SemaphoreType.DMA((2, groups, 4)),
            pltpu.SemaphoreType.DMA((2, groups, 4)),
        ],
        compiler_params=pltpu.CompilerParams(
            collective_id=0, has_side_effects=True, vmem_limit_bytes=60 * 1024 * 1024
        ),
    )(wind, field, inverse, mixing)


def gather_kernel(payload, out, send_sem, recv_sem):
    n_gy = lax.axis_size("gy")
    devices = lax.axis_size("gx") * n_gy
    me = lax.axis_index("gx") * n_gy + lax.axis_index("gy")

    def place(k):
        other = (me + k) % devices
        return (other // n_gy, other % n_gy)

    def greet(k, carry):
        pl.semaphore_signal(
            pltpu.get_barrier_semaphore(), inc=1, device_id=place(k), device_id_type=pl.DeviceIdType.MESH
        )
        return carry

    lax.fori_loop(1, devices, greet, 0)
    pl.semaphore_wait(pltpu.get_barrier_semaphore(), devices - 1)

    def copy(k, slot):
        return pltpu.make_async_remote_copy(
            src_ref=payload,
            dst_ref=out.at[slot],
            send_sem=send_sem.at[k],
            recv_sem=recv_sem.at[k],
            device_id=place(k),
            device_id_type=pl.DeviceIdType.MESH,
        )

    def send(k, carry):
        copy(k, me).start()
        return carry

    def finish(k, carry):
        arriving = copy(k, (me + devices - k) % devices)
        arriving.wait_send()
        arriving.wait_recv()
        return carry

    lax.fori_loop(1, devices, send, 0)
    out[me] = payload[...]
    lax.fori_loop(1, devices, finish, 0)


def gather_all(payload):
    devices = lax.axis_size("gx") * lax.axis_size("gy")
    vmem = pl.BlockSpec(memory_space=pltpu.VMEM)
    return pl.pallas_call(
        gather_kernel,
        out_shape=jax.ShapeDtypeStruct((devices,) + payload.shape, jnp.float32),
        in_specs=[vmem],
        out_specs=vmem,
        scratch_shapes=[pltpu.SemaphoreType.DMA((devices,)), pltpu.SemaphoreType.DMA((devices,))],
        compiler_params=pltpu.CompilerParams(collective_id=1, has_side_effects=True),
    )(payload)


def body(probes, diffusivity, wind_speed, sensor_cell, sensor_owner, sensor_count, goal_weight):
    probe_count, nx, ny, nz = probes.shape
    groups = probe_count // LANES
    field = probes.reshape(groups, LANES, nx, ny, nz).transpose(0, 2, 3, 1, 4)
    inverse = 1.0 / (
        1.0 + time_step * (6.0 * diffusivity + wind_speed[0] + wind_speed[1] + wind_speed[2])
    )
    mixing = time_step * diffusivity * inverse
    wide = (nx, ny, LANES, nz)
    state = run_sweeps(
        time_step * wind_speed,
        field,
        jnp.broadcast_to(inverse[:, :, None, :], wide),
        jnp.broadcast_to(mixing[:, :, None, :], wide),
    )
    fields = state.transpose(0, 3, 1, 2, 4).reshape(probes.shape)

    sensor_rows = sensor_cell.shape[2]
    goal_count = goal_weight.shape[3]
    device_count = lax.axis_size("gx") * lax.axis_size("gy")
    cells = sensor_cell.reshape(-1)
    columns = jnp.take(state.reshape(groups, nx * ny, LANES, nz), cells // nz, axis=1, mode="clip")
    here = jnp.arange(nz, dtype=jnp.int32)[None, :] == (cells % nz)[:, None]
    readings = jnp.sum(jnp.where(here[None, :, None, :], columns, 0.0), axis=3)
    readings = readings.transpose(1, 0, 2).reshape(sensor_rows, probe_count)
    active = jnp.arange(sensor_rows, dtype=jnp.int32) < sensor_count.reshape(())
    readings = jnp.where(active[:, None], readings, 0.0)
    payload = jnp.concatenate(
        [
            readings,
            goal_weight.reshape(sensor_rows, goal_count),
            sensor_owner.reshape(sensor_rows, 1).astype(jnp.float32),
        ],
        axis=1,
    )
    width = payload.shape[1]
    payload = jnp.pad(payload.T, ((0, -width % 8), (0, 0)))
    everyone = gather_all(payload).transpose(0, 2, 1).reshape(device_count * sensor_rows, -1)
    all_readings = everyone[:, :probe_count]
    all_weights = everyone[:, probe_count : probe_count + goal_count]
    owners = everyone[:, probe_count + goal_count].astype(jnp.int32)
    onehot = (owners[:, None] == jnp.arange(device_count, dtype=jnp.int32)[None, :]).astype(jnp.float32)
    outer = (all_weights[:, :, None] * all_readings[:, None, :]).reshape(-1, goal_count * probe_count)
    goals = jnp.dot(onehot.T, outer, precision=lax.Precision.HIGHEST)
    goals = goals.reshape(device_count * goal_count, probe_count)
    ritz_gram = jnp.dot(goals.T, goals, precision=lax.Precision.HIGHEST)
    mine = lax.axis_index("gx") * lax.axis_size("gy") + lax.axis_index("gy")
    goal_block = lax.dynamic_slice_in_dim(goals, mine * goal_count, goal_count, axis=0)
    return (fields, goal_block, ritz_gram)


def solution(mesh):
    placed = (
        P(None, "gx", "gy", None),
        P("gx", "gy", None),
        P(),
        P("gx", "gy", None),
        P("gx", "gy", None, None),
        P("gx", "gy"),
        P("gx", "gy", None, None),
    )
    return jax.shard_map(
        body,
        mesh=mesh,
        in_specs=placed,
        out_specs=(P(None, "gx", "gy", None), P(("gx", "gy"), None), P()),
        check_vma=False,
    )
```
